32 devices in a mesh: gx: 16 (over z, y, core), gy: 2 (over x).
Axes of the slice: x: 2, y: 2, z: 4, core: 2. Of those that a mesh axis runs over, the one named last changes fastest.
Arguments:
- old_block: float32 [12288, 24576], P('gx', 'gy'), may hold values from -6 to 6
- vectors: bfloat16 [256, 2, 12288], P(None, 'gy', 'gx'), may hold values from -4 to 4
- prior: bfloat16 [32768, 3072], P('gx', 'gy'), may hold values from -2 to 2
- pair_columns: float32 [32768, 128], P(('gx', 'gy')), may hold values from -6 to 6
- pivots: int32 [128], replicated, may hold values from 0 to 32767
Outputs:
- new_block: float32 [12288, 24576], P('gx', 'gy')
- residual_columns: float32 [32768, 128], P(('gx', 'gy'))
The draws below stay inside these ranges and needn't reach their ends.
Inputs may be any that keep to these rules, and one draw needn't show every extreme that they name: `pivots`: pivot AO-pair row indices, repeats possible.
All inputs are finite; a program needn't handle non-finite values.
Results may differ from the reference program's by a relative error of at most 0.0055.
Values may be sent and summed in bfloat16 or wider, within the bound.
A program may use at most 192 MiB of HBM per device.

```python
import jax
import jax.numpy as jnp
from jax import lax

NVEC = 256
NPRIOR = 3072
NPIV = 128
NIA = 24576
SLAB = 12288
NPAIR = 32768
N_GY = 2


def plant(entries, stream_key, low, largest):
    longest = entries.shape.index(max(entries.shape))
    spots = []
    for shift in (0, 1):
        where = [jax.random.randint(jax.random.fold_in(stream_key, axis), (), 0, length) for axis, length in enumerate(entries.shape)]
        where[longest] = (where[longest] + shift) % entries.shape[longest]
        spots.append(tuple(where))
    return entries.at[spots[0]].set(low).at[spots[1]].set(largest)


def block_levels(own_key, extent, split, least, largest):
    level = 1.0
    for axis_at, shards_of in split:
        steps = jax.random.uniform(jax.random.fold_in(jax.random.fold_in(own_key, 6), axis_at), (shards_of,), jnp.float32, least / len(split), largest / len(split))
        level = level * jnp.repeat(jnp.exp(steps), extent[axis_at] // shards_of).reshape((-1,) + (1,) * (len(extent) - 1 - axis_at))
    return level


def scatter_about(own_key, extent, deviation, bound, split=(), held_as=jnp.bfloat16):
    drawn = jax.random.normal(own_key, extent, jnp.float32) * deviation
    if len(split) > 0:
        drawn = block_levels(own_key, extent, split, -0.22, 0.18) * drawn
    return jnp.clip(drawn, min=-bound, max=bound).astype(held_as)


def setup_inputs(seed: int = 0) -> dict:
    streams_of = jax.random.split(jax.random.key(seed), 6)
    old_block = scatter_about(streams_of[0], (SLAB, NIA), 1.0, 6.0, ((0, 16), (1, 2)), jnp.float32)
    vectors = scatter_about(streams_of[1], (NVEC, N_GY, NIA // N_GY), (NVEC ** -0.25), 4.0, ((1, 2), (2, 16)))
    prior = scatter_about(streams_of[2], (NPAIR, NPRIOR), (NPRIOR ** -0.25), 2.0, ((0, 16), (1, 2)))
    pair_columns = scatter_about(streams_of[3], (NPAIR, NPIV), 1.0, 6.0, ((0, 32),), jnp.float32)
    pivots = plant(jax.random.randint(streams_of[4], (NPIV,), 0, NPAIR), jax.random.fold_in(streams_of[4], 1), 0, NPAIR - 1).astype(jnp.int32)
    return dict(old_block=old_block, vectors=vectors, prior=prior, pair_columns=pair_columns, pivots=pivots)


def reference(old_block, vectors, prior, pair_columns, pivots):
    flat = vectors.reshape(NVEC, NIA)
    slab = NIA // N_GY
    new_block = old_block + jnp.dot(flat[:, :slab].T, flat, preferred_element_type=jnp.float32)
    picked = jnp.take(prior, pivots, axis=0)
    width = NPRIOR // N_GY
    intersection = jnp.zeros((prior.shape[0], NPIV), jnp.float32)
    for group in range(N_GY):
        part = jnp.dot(prior[:, group * width:(group + 1) * width], picked[:, group * width:(group + 1) * width].T, preferred_element_type=jnp.float32)
        rounded = lax.optimization_barrier(part.astype(jnp.bfloat16))
        intersection = intersection + rounded.astype(jnp.float32)
    return new_block, pair_columns - intersection
```

```python
import functools

import jax
import jax.numpy as jnp
from jax import lax
from jax.experimental import pallas as pl
from jax.experimental.pallas import tpu as pltpu
from jax.sharding import PartitionSpec as P

F32 = jnp.float32
BF16 = jnp.bfloat16
MESH = pl.DeviceIdType.MESH


def from_root(value, axis, root):
    mine = lax.axis_index(axis) == root
    return lax.psum(jnp.where(mine, value, jnp.zeros_like(value)), axis)


def plain(old_block, vectors, prior, pair_columns, pivots):
    local_vectors = vectors.reshape(vectors.shape[0], vectors.shape[2])
    slab_part = from_root(local_vectors, "gy", 0)
    gained = jnp.dot(slab_part.T, lax.all_gather(local_vectors, "gx", axis=1, tiled=True), preferred_element_type=F32)
    new_block = old_block + gained
    rows_local = prior.shape[0]
    local_index = pivots - lax.axis_index("gx") * rows_local
    inside = jnp.logical_and(local_index >= 0, local_index < rows_local)
    chosen = jnp.take(prior, jnp.clip(local_index, 0, rows_local - 1), axis=0)
    chosen = jnp.where(inside[:, None], chosen, jnp.zeros_like(chosen))
    pivot_block = lax.psum(chosen, "gx")
    part = jnp.dot(prior, pivot_block.T, preferred_element_type=F32).astype(BF16)
    parts = lax.all_to_all(part.reshape(lax.axis_size("gy"), -1, part.shape[1]), "gy", split_axis=0, concat_axis=0)
    rounded = lax.optimization_barrier(parts)
    return new_block, pair_columns - jnp.sum(rounded.astype(F32), axis=0)


def kernel(n, m, vec_ref, prior_ref, old_ref, pair_ref, piv_ref, acc, resid, held, slab, slab_t, prior, wide, chosen,
           half_in, half, rs_in, pick, parts, parts_in, vec_sem, prior_sem, old_sem, own_sem,
           v_send, v_recv, s_send, s_recv, d_send, d_recv, rs_send, rs_recv, ag_send, ag_recv, p_send, p_recv):
    depth, width = vec_ref.shape
    line = n // 4
    chips = n // 2
    gx, gy = lax.axis_index("gx"), lax.axis_index("gy")
    pos, y, core = gx // 4, lax.rem(gx // 2, 2), lax.rem(gx, 2)
    chip = gx // 2
    rows_of = prior.shape[0] // m
    each = chosen.shape[2]

    def at(p, yy, c):
        return (p * 2 + yy) * 2 + c

    prior_in = pltpu.make_async_copy(prior_ref, prior, prior_sem)
    vec_in = pltpu.make_async_copy(vec_ref, held.at[gx], vec_sem)
    vec_in.start()
    prior_in.start()

    def old_copy(block):
        columns = pl.ds(pl.multiple_of(block * width, 128), width)
        return pltpu.make_async_copy(old_ref.at[:, columns], acc.at[:, columns], old_sem.at[block])

    barrier = pltpu.get_barrier_semaphore()
    for step in range(1, n):
        pl.semaphore_signal(barrier, inc=1, device_id=(lax.rem(gx + step, n), gy), device_id_type=MESH)
    for step in range(1, m):
        pl.semaphore_signal(barrier, inc=1, device_id=(gx, lax.rem(gy + step, m)), device_id_type=MESH)
    pl.semaphore_wait(barrier, n - 1 + m - 1)

    sent = []

    def send(copy, when=None):
        def begin():
            copy.start()
        if when is None:
            begin()
        else:
            pl.when(when)(begin)
        sent.append((copy, when))

    def block_copy(src, way, target):
        return pltpu.make_async_remote_copy(held.at[src], held.at[src], v_send.at[src, way], v_recv.at[src], device_id=(target, gy), device_id_type=MESH)

    def arrived(src):
        block_copy(src, 0, gx).wait_recv()

    vec_in.wait()
    send(block_copy(gx, 0, at(pos + 1, y, core)), pos + 1 < line)
    send(block_copy(gx, 1, at(pos - 1, y, core)), pos > 0)
    send(block_copy(gx, 2, at(pos, 1 - y, core)))
    for step in range(1, m):
        copy = pltpu.make_async_remote_copy(held.at[gx], slab, s_send.at[step - 1], s_recv, device_id=(gx, lax.rem(gy + step, m)), device_id_type=MESH)
        send(copy, gy == 0)
    send(block_copy(gx, 3, at(pos, y, 1 - core)))

    prior_in.wait()
    for step in range(n):
        old_copy(step).start()
    local_index = piv_ref[...] - chip_rows(gx, prior)
    onehot = (lax.broadcasted_iota(jnp.int32, (piv_ref.shape[0], prior.shape[0]), 1) == local_index).astype(F32).astype(BF16)
    tile = 256

    def pick_tile(i, _):
        columns = pl.ds(pl.multiple_of(i * tile, tile), tile)
        wide[:, columns] = jnp.dot(onehot, prior[:, columns], preferred_element_type=F32)
        return 0
    lax.fori_loop(0, prior.shape[1] // tile, pick_tile, 0)
    for i in range(n):
        chosen[i // chips, i % chips] = wide[i * each:(i + 1) * each, :].astype(BF16)
    first = pltpu.make_async_remote_copy(chosen.at[1 - core], half_in, d_send.at[0], d_recv.at[0], device_id=(at(pos, y, 1 - core), gy), device_id_type=MESH)

    @pl.when(gy == 0)
    def _():
        own = pltpu.make_async_copy(vec_ref, slab, own_sem)
        own.start()
        own.wait()
    send(first)

    first.wait_recv()
    for i in range(chips):
        half[i] = (chosen[core, i].astype(F32) + half_in[i].astype(F32)).astype(BF16)

    def line_round(step):
        for way, src_pos, ok in ((0, pos - step, pos - step >= 0), (1, pos + step, pos + step < line)):
            src = at(src_pos, y, core)

            @pl.when(ok)
            def _():
                arrived(src)
            onward = pos + 1 if way == 0 else pos - 1
            more = jnp.logical_and(ok, onward < line) if way == 0 else jnp.logical_and(ok, onward >= 0)
            send(block_copy(src, 2, at(pos, 1 - y, core)), ok)
            send(block_copy(src, way, at(onward, y, core)), more)
            send(block_copy(src, 3, at(pos, y, 1 - core)), ok)

    def over_y(src_pos, ok):
        src = at(src_pos, 1 - y, core)

        def go():
            arrived(src)
            block_copy(src, 3, at(pos, y, 1 - core)).start()
        if ok is None:
            go()
        else:
            pl.when(ok)(go)
        sent.append((block_copy(src, 3, at(pos, y, 1 - core)), ok))

    def update(block):
        old_copy(block).wait()
        columns = pl.ds(pl.multiple_of(block * width, 128), width)

        def rows_step(i, _):
            rows = pl.ds(pl.multiple_of(i * tile, tile), tile)
            acc[rows, columns] += jnp.dot(slab_t[rows, :], held[block], preferred_element_type=F32)
            return 0
        lax.fori_loop(0, acc.shape[0] // tile, rows_step, 0)

    def updates(src_pos, yy, c, ok, wait):
        def go():
            src = at(src_pos, yy, c)
            if wait:
                arrived(src)
            update(src)
        if ok is None:
            go()
        else:
            pl.when(ok)(go)

    for step in range(1, chips):
        other = lax.rem(chip + step, chips)
        send(pltpu.make_async_remote_copy(half.at[other], rs_in.at[step - 1], rs_send.at[step - 1], rs_recv.at[step - 1], device_id=(other * 2 + core, gy), device_id_type=MESH))

    line_round(1)

    total = half[chip].astype(F32)
    for step in range(1, chips):
        pltpu.make_async_remote_copy(half.at[chip], rs_in.at[step - 1], rs_send.at[step - 1], rs_recv.at[step - 1], device_id=(gx, gy), device_id_type=MESH).wait_recv()
        total = total + rs_in[step - 1].astype(F32)
    pick[core, chip] = total.astype(BF16)

    @pl.when(gy != 0)
    def _():
        pltpu.make_async_remote_copy(held.at[gx], slab, s_send.at[0], s_recv, device_id=(gx, gy), device_id_type=MESH).wait_recv()
    slab_t[...] = slab[...].T

    for step in range(1, chips):
        other = lax.rem(chip + step, chips)
        send(pltpu.make_async_remote_copy(pick.at[core, chip], pick.at[core, chip], ag_send.at[step - 1], ag_recv.at[step - 1], device_id=(other * 2 + core, gy), device_id_type=MESH))

    over_y(pos, None)
    updates(pos, y, core, None, False)
    updates(pos, y, 1 - core, None, True)
    for src_pos, ok in ((pos - 1, pos >= 1), (pos + 1, pos + 1 < line)):
        updates(src_pos, y, core, ok, False)

    line_round(2)
    for step in range(1, chips):
        other = lax.rem(chip + chips - step, chips)
        pltpu.make_async_remote_copy(pick.at[core, other], pick.at[core, other], ag_send.at[step - 1], ag_recv.at[step - 1], device_id=(gx, gy), device_id_type=MESH).wait_recv()
    last = pltpu.make_async_remote_copy(pick.at[core], pick.at[core], d_send.at[1], d_recv.at[1], device_id=(at(pos, y, 1 - core), gy), device_id_type=MESH)
    send(last)
    for src_pos, ok in ((pos - 1, pos >= 1), (pos + 1, pos + 1 < line)):
        over_y(src_pos, ok)
        updates(src_pos, y, 1 - core, ok, True)
    updates(pos, 1 - y, core, None, False)
    updates(pos, 1 - y, 1 - core, None, True)

    pltpu.make_async_remote_copy(pick.at[1 - core], pick.at[1 - core], d_send.at[1], d_recv.at[1], device_id=(gx, gy), device_id_type=MESH).wait_recv()
    for i in range(n):
        wide[i * each:(i + 1) * each, :] = pick[i // chips, i % chips].astype(F32)
    picked = wide[...].astype(BF16)

    def part_rows(g):
        def go(i, _):
            rows = pl.ds(pl.multiple_of(i * tile, tile), tile)
            source = pl.ds(pl.multiple_of(g * rows_of + i * tile, tile), tile)
            parts[g, rows, :] = lax.dot_general(prior[source, :], picked, (((1,), (1,)), ((), ())), preferred_element_type=F32).astype(BF16)
            return 0
        lax.fori_loop(0, rows_of // tile, go, 0)

    for g in range(m):
        part_rows(g)

    for step in range(2, line):
        if step > 2:
            line_round(step)
        if step == 2:
            for k in range(1, m):
                to = lax.rem(gy + k, m)
                send(pltpu.make_async_remote_copy(parts.at[to], parts_in.at[k - 1], p_send.at[k - 1], p_recv.at[k - 1], device_id=(gx, to), device_id_type=MESH))
        for src_pos, ok in ((pos - step, pos >= step), (pos + step, pos + step < line)):
            updates(src_pos, y, core, ok, False)
            updates(src_pos, y, 1 - core, ok, True)
        before = step - 1
        for src_pos, ok in ((pos - before, pos >= before), (pos + before, pos + before < line)):
            updates(src_pos, 1 - y, core, ok, False)
            updates(src_pos, 1 - y, 1 - core, ok, True)
        for src_pos, ok in ((pos - step, pos >= step), (pos + step, pos + step < line)):
            over_y(src_pos, ok)
    step = line - 1
    for src_pos, ok in ((pos - step, pos >= step), (pos + step, pos + step < line)):
        updates(src_pos, 1 - y, core, ok, False)
        updates(src_pos, 1 - y, 1 - core, ok, True)

    total = parts[gy].astype(F32)
    for k in range(1, m):
        pltpu.make_async_remote_copy(parts.at[gy], parts_in.at[k - 1], p_send.at[k - 1], p_recv.at[k - 1], device_id=(gx, gy), device_id_type=MESH).wait_recv()
        total = total + parts_in[k - 1].astype(F32)
    resid[...] = pair_ref[...] - total

    for copy, when in sent:
        if when is None:
            copy.wait_send()
        else:
            pl.when(when)(copy.wait_send)


def chip_rows(gx, prior):
    return gx * prior.shape[0]


def fused(n, m, old_block, vectors, prior, pair_columns, pivots):
    depth, width = vectors.shape[0], vectors.shape[2]
    rows, columns = old_block.shape
    keys, prior_width = pivots.shape[0], prior.shape[1]
    each, chips = keys // n, n // 2
    rows_of = prior.shape[0] // m
    dma = pltpu.SemaphoreType.DMA
    anywhere = pl.BlockSpec(memory_space=pl.ANY)
    vmem = pl.BlockSpec(memory_space=pltpu.VMEM)
    return pl.pallas_call(
        functools.partial(kernel, n, m),
        out_shape=(pltpu.VMEM((rows, columns), F32), jax.ShapeDtypeStruct(pair_columns.shape, F32)),
        in_specs=[anywhere, anywhere, anywhere, vmem, vmem],
        out_specs=(vmem, vmem),
        scratch_shapes=[
            pltpu.VMEM((n, depth, width), BF16),
            pltpu.VMEM((depth, width), BF16),
            pltpu.VMEM((width, depth), BF16),
            pltpu.VMEM(prior.shape, BF16),
            pltpu.VMEM((keys, prior_width), F32),
            pltpu.VMEM((2, chips, each, prior_width), BF16),
            pltpu.VMEM((chips, each, prior_width), BF16),
            pltpu.VMEM((chips, each, prior_width), BF16),
            pltpu.VMEM((chips - 1, each, prior_width), BF16),
            pltpu.VMEM((2, chips, each, prior_width), BF16),
            pltpu.VMEM((m, rows_of, keys), BF16),
            pltpu.VMEM((m - 1, rows_of, keys), BF16),
            dma, dma, dma((n,)), dma,
            dma((n, 4)), dma((n,)), dma((m - 1,)), dma, dma((2,)), dma((2,)),
            dma((chips - 1,)), dma((chips - 1,)), dma((chips - 1,)), dma((chips - 1,)), dma((m - 1,)), dma((m - 1,)),
        ],
        compiler_params=pltpu.CompilerParams(collective_id=0, has_side_effects=True, vmem_limit_bytes=VMEM_LIMIT),
    )(vectors.reshape(depth, width), prior, old_block, pair_columns, pivots.reshape(keys, 1))


VMEM_LIMIT = 26 * 1024 * 1024


def solution(mesh):
    n, m = mesh.shape["gx"], mesh.shape["gy"]

    def local(old_block, vectors, prior, pair_columns, pivots):
        width = vectors.shape[2]
        whole_tiles = width % 256 == 0 and prior.shape[1] % 256 == 0 and prior.shape[0] // m % 256 == 0
        if n % 4 == 0 and n >= 12 and m >= 2 and pivots.shape[0] % (8 * n) == 0 and whole_tiles:
            return fused(n, m, old_block, vectors, prior, pair_columns, pivots)
        return plain(old_block, vectors, prior, pair_columns, pivots)

    placed = (P("gx", "gy"), P(None, "gy", "gx"), P("gx", "gy"), P(("gx", "gy"), None), P())
    return jax.shard_map(
        local,
        mesh=mesh,
        in_specs=placed,
        out_specs=(P("gx", "gy"), P(("gx", "gy"), None)),
        check_vma=False,
    )
```

```python
import functools

import jax
import jax.numpy as jnp
from jax import lax
from jax.experimental import pallas as pl
from jax.experimental.pallas import tpu as pltpu
from jax.sharding import PartitionSpec as P

F32 = jnp.float32
BF16 = jnp.bfloat16
MESH = pl.DeviceIdType.MESH


def from_root(value, axis, root):
    mine = lax.axis_index(axis) == root
    return lax.psum(jnp.where(mine, value, jnp.zeros_like(value)), axis)


def plain(old_block, vectors, prior, pair_columns, pivots):
    local_vectors = vectors.reshape(vectors.shape[0], vectors.shape[2])
    slab_part = from_root(local_vectors, "gy", 0)
    gained = jnp.dot(slab_part.T, lax.all_gather(local_vectors, "gx", axis=1, tiled=True), preferred_element_type=F32)
    new_block = old_block + gained
    rows_local = prior.shape[0]
    local_index = pivots - lax.axis_index("gx") * rows_local
    inside = jnp.logical_and(local_index >= 0, local_index < rows_local)
    chosen = jnp.take(prior, jnp.clip(local_index, 0, rows_local - 1), axis=0)
    chosen = jnp.where(inside[:, None], chosen, jnp.zeros_like(chosen))
    pivot_block = lax.psum(chosen, "gx")
    part = jnp.dot(prior, pivot_block.T, preferred_element_type=F32).astype(BF16)
    parts = lax.all_to_all(part.reshape(lax.axis_size("gy"), -1, part.shape[1]), "gy", split_axis=0, concat_axis=0)
    rounded = lax.optimization_barrier(parts)
    return new_block, pair_columns - jnp.sum(rounded.astype(F32), axis=0)


def kernel(n, m, pieces, vec_ref, prior_ref, old_ref, pair_ref, piv_ref, acc, resid, held, slab_t, slab, prior, wide, chosen,
           half_in, half, rs_in, pick, parts, parts_in, vec_sem, prior_sem, old_sem, own_sem,
           v_send, v_recv, s_send, s_recv, d_send, d_recv, rs_send, rs_recv, ag_send, ag_recv, p_send, p_recv):
    depth, width = vec_ref.shape
    line = n // 4
    chips = n // 2
    gx, gy = lax.axis_index("gx"), lax.axis_index("gy")
    pos, y, core = gx // 4, lax.rem(gx // 2, 2), lax.rem(gx, 2)
    chip = gx // 2
    rows_of = prior.shape[0] // m
    each = chosen.shape[2]
    tile = 256
    by_line, by_y = range(len(pieces) - 1), len(pieces) - 1

    def at(p, yy, c):
        return (p * 2 + yy) * 2 + c

    prior_in = pltpu.make_async_copy(prior_ref, prior, prior_sem)
    vec_in = pltpu.make_async_copy(vec_ref, held.at[gx], vec_sem)
    vec_in.start()
    prior_in.start()

    def old_copy(block):
        columns = pl.ds(pl.multiple_of(block * width, 128), width)
        return pltpu.make_async_copy(old_ref.at[:, columns], acc.at[:, columns], old_sem.at[block])

    barrier = pltpu.get_barrier_semaphore()
    for step in range(1, n):
        pl.semaphore_signal(barrier, inc=1, device_id=(lax.rem(gx + step, n), gy), device_id_type=MESH)
    for step in range(1, m):
        pl.semaphore_signal(barrier, inc=1, device_id=(gx, lax.rem(gy + step, m)), device_id_type=MESH)
    pl.semaphore_wait(barrier, n - 1 + m - 1)

    sent = []

    def send(copy, when=None):
        if when is None:
            copy.start()
        else:
            pl.when(when)(copy.start)
        sent.append((copy, when))

    def ways(p, yy, c):
        return at(p + 1, yy, c), at(p - 1, yy, c), at(p, 1 - yy, c), at(p, yy, 1 - c)

    targets = ways(pos, y, core)

    def piece_copy(src, piece, way):
        first_row, count = pieces[piece]
        part = held.at[src, pl.ds(first_row, count)]
        return pltpu.make_async_remote_copy(part, part, v_send.at[src, piece, way], v_recv.at[src, piece], device_id=(targets[way], gy), device_id_type=MESH)

    def arrived(src, piece):
        piece_copy(src, piece, 3).wait_recv()

    vec_in.wait()
    send(piece_copy(gx, by_y, 2))
    for piece in (*by_line, by_y):
        send(piece_copy(gx, piece, 0), pos + 1 < line)
        send(piece_copy(gx, piece, 1), pos > 0)
        if piece != by_y:
            send(piece_copy(gx, piece, 2))
    for step in range(1, m):
        copy = pltpu.make_async_remote_copy(held.at[gx], slab, s_send.at[step - 1], s_recv, device_id=(gx, lax.rem(gy + step, m)), device_id_type=MESH)
        send(copy, gy == 0)
    for piece in (*by_line, by_y):
        send(piece_copy(gx, piece, 3))

    prior_in.wait()
    for step in range(n):
        old_copy(step).start()
    keys = piv_ref.shape[1]
    local_index = jnp.broadcast_to(piv_ref[...], (keys, keys)).T[:, :1] - gx * prior.shape[0]
    onehot = (lax.broadcasted_iota(jnp.int32, (keys, prior.shape[0]), 1) == local_index).astype(F32).astype(BF16)

    def pick_tile(i, _):
        columns = pl.ds(pl.multiple_of(i * tile, tile), tile)
        wide[:, columns] = jnp.dot(onehot, prior[:, columns], preferred_element_type=F32)
        return 0
    lax.fori_loop(0, prior.shape[1] // tile, pick_tile, 0)
    for i in range(n):
        chosen[i // chips, i % chips] = wide[i * each:(i + 1) * each, :].astype(BF16)

    @pl.when(gy == 0)
    def _():
        own = pltpu.make_async_copy(vec_ref, slab, own_sem)
        own.start()
        own.wait()
    first = pltpu.make_async_remote_copy(chosen.at[1 - core], half_in, d_send.at[0], d_recv.at[0], device_id=(targets[3], gy), device_id_type=MESH)
    send(first)

    across = at(pos, 1 - y, core)
    arrived(across, by_y)
    send(piece_copy(across, by_y, 0), pos + 1 < line)
    send(piece_copy(across, by_y, 1), pos > 0)
    send(piece_copy(across, by_y, 3))

    first.wait_recv()
    for i in range(chips):
        half[i] = (chosen[core, i].astype(F32) + half_in[i].astype(F32)).astype(BF16)

    def sides(step):
        return ((0, pos - step, pos >= step), (1, pos + step, pos + step < line))

    def line_round(step, piece, yy, on_y):
        for way, src_pos, ok in sides(step):
            src = at(src_pos, yy, core)

            @pl.when(ok)
            def _():
                arrived(src, piece)
            onward = pos + 1 < line if way == 0 else pos > 0
            send(piece_copy(src, piece, way), jnp.logical_and(ok, onward))
            if on_y:
                send(piece_copy(src, piece, 2), ok)
            send(piece_copy(src, piece, 3), ok)

    def over_y(src_pos, ok):
        src = at(src_pos, 1 - y, core)
        for piece in by_line:
            if ok is None:
                arrived(src, piece)
            else:
                pl.when(ok)(functools.partial(arrived, src, piece))
            send(piece_copy(src, piece, 3), ok)

    def update(block):
        columns = pl.ds(pl.multiple_of(block * width, 128), width)

        def rows_step(i, _):
            rows = pl.ds(pl.multiple_of(i * tile, tile), tile)
            acc[rows, columns] += jnp.dot(slab_t[rows, :], held[block], preferred_element_type=F32)
            return 0
        lax.fori_loop(0, acc.shape[0] // tile, rows_step, 0)

    def updates(src_pos, yy, c, ok, wait):
        def go():
            src = at(src_pos, yy, c)
            if wait:
                for piece in range(len(pieces)):
                    arrived(src, piece)
            old_copy(src).wait()
            update(src)
        if ok is None:
            go()
        else:
            pl.when(ok)(go)

    for step in range(1, chips):
        other = lax.rem(chip + step, chips)
        send(pltpu.make_async_remote_copy(half.at[other], rs_in.at[step - 1], rs_send.at[step - 1], rs_recv.at[step - 1], device_id=(other * 2 + core, gy), device_id_type=MESH))

    for piece in by_line:
        line_round(1, piece, y, True)
    line_round(1, by_y, y, False)

    @pl.when(gy != 0)
    def _():
        pltpu.make_async_remote_copy(held.at[gx], slab, s_send.at[0], s_recv, device_id=(gx, gy), device_id_type=MESH).wait_recv()
    slab_t[...] = slab[...].T
    updates(pos, y, core, None, False)
    line_round(1, by_y, 1 - y, False)
    updates(pos, y, 1 - core, None, True)

    total = half[chip].astype(F32)
    for step in range(1, chips):
        pltpu.make_async_remote_copy(half.at[chip], rs_in.at[step - 1], rs_send.at[step - 1], rs_recv.at[step - 1], device_id=(gx, gy), device_id_type=MESH).wait_recv()
        total = total + rs_in[step - 1].astype(F32)
    pick[core, chip] = total.astype(BF16)

    over_y(pos, None)
    line_round(2, by_line[0], y, True)

    for step in range(1, chips):
        other = lax.rem(chip + step, chips)
        send(pltpu.make_async_remote_copy(pick.at[core, chip], pick.at[core, chip], ag_send.at[step - 1], ag_recv.at[step - 1], device_id=(other * 2 + core, gy), device_id_type=MESH))

    for way, src_pos, ok in sides(1):
        updates(src_pos, y, core, ok, False)
    for piece in by_line[1:]:
        line_round(2, piece, y, True)
    line_round(2, by_y, y, False)
    line_round(2, by_y, 1 - y, False)
    updates(pos, 1 - y, core, None, False)
    for way, src_pos, ok in sides(1):
        over_y(src_pos, ok)
        updates(src_pos, y, 1 - core, ok, True)

    for step in range(1, chips):
        other = lax.rem(chip + chips - step, chips)
        pltpu.make_async_remote_copy(pick.at[core, other], pick.at[core, other], ag_send.at[step - 1], ag_recv.at[step - 1], device_id=(gx, gy), device_id_type=MESH).wait_recv()
    last = pltpu.make_async_remote_copy(pick.at[core], pick.at[core], d_send.at[1], d_recv.at[1], device_id=(targets[3], gy), device_id_type=MESH)
    send(last)
    updates(pos, 1 - y, 1 - core, None, True)

    for step in range(3, line):
        for piece in by_line:
            line_round(step, piece, y, True)
        line_round(step, by_y, y, False)
        line_round(step, by_y, 1 - y, False)

    pltpu.make_async_remote_copy(pick.at[1 - core], pick.at[1 - core], d_send.at[1], d_recv.at[1], device_id=(gx, gy), device_id_type=MESH).wait_recv()
    for i in range(n):
        wide[i * each:(i + 1) * each, :] = pick[i // chips, i % chips].astype(F32)
    picked = wide[...].astype(BF16)

    def part_rows(g):
        def go(i, _):
            rows = pl.ds(pl.multiple_of(i * tile, tile), tile)
            source = pl.ds(pl.multiple_of(g * rows_of + i * tile, tile), tile)
            parts[g, rows, :] = lax.dot_general(prior[source, :], picked, (((1,), (1,)), ((), ())), preferred_element_type=F32).astype(BF16)
            return 0
        lax.fori_loop(0, rows_of // tile, go, 0)

    for g in range(m):
        part_rows(g)
    for way, src_pos, ok in sides(1):
        updates(src_pos, 1 - y, core, ok, False)
    for k in range(1, m):
        to = lax.rem(gy + k, m)
        send(pltpu.make_async_remote_copy(parts.at[to], parts_in.at[k - 1], p_send.at[k - 1], p_recv.at[k - 1], device_id=(gx, to), device_id_type=MESH))
    for way, src_pos, ok in sides(1):
        updates(src_pos, 1 - y, 1 - core, ok, True)

    for step in range(2, line):
        for way, src_pos, ok in sides(step):
            updates(src_pos, y, core, ok, False)
            over_y(src_pos, ok)
            updates(src_pos, y, 1 - core, ok, True)
        for way, src_pos, ok in sides(step):
            updates(src_pos, 1 - y, core, ok, False)
            if step < line - 1:
                updates(src_pos, 1 - y, 1 - core, ok, True)

    total = parts[gy].astype(F32)
    for k in range(1, m):
        pltpu.make_async_remote_copy(parts.at[gy], parts_in.at[k - 1], p_send.at[k - 1], p_recv.at[k - 1], device_id=(gx, gy), device_id_type=MESH).wait_recv()
        total = total + parts_in[k - 1].astype(F32)
    resid[...] = pair_ref[...] - total
    for way, src_pos, ok in sides(line - 1):
        updates(src_pos, 1 - y, 1 - core, ok, True)

    for copy, when in sent:
        if when is None:
            copy.wait_send()
        else:
            pl.when(when)(copy.wait_send)


def fused(n, m, old_block, vectors, prior, pair_columns, pivots):
    depth, width = vectors.shape[0], vectors.shape[2]
    rows, columns = old_block.shape
    keys, prior_width = pivots.shape[0], prior.shape[1]
    each, chips = keys // n, n // 2
    rows_of = prior.shape[0] // m
    unit = depth // 16
    pieces = ((0, 6 * unit), (6 * unit, 7 * unit), (13 * unit, depth - 13 * unit))
    dma = pltpu.SemaphoreType.DMA
    anywhere = pl.BlockSpec(memory_space=pl.ANY)
    vmem = pl.BlockSpec(memory_space=pltpu.VMEM)
    return pl.pallas_call(
        functools.partial(kernel, n, m, pieces),
        out_shape=(
            pltpu.VMEM((rows, columns), F32),
            jax.ShapeDtypeStruct(pair_columns.shape, F32),
        ),
        in_specs=[anywhere, anywhere, anywhere, vmem, vmem],
        out_specs=(vmem, vmem),
        scratch_shapes=[
            pltpu.VMEM((n, depth, width), BF16),
            pltpu.VMEM((width, depth), BF16),
            pltpu.VMEM((depth, width), BF16),
            pltpu.VMEM(prior.shape, BF16),
            pltpu.VMEM((keys, prior_width), F32),
            pltpu.VMEM((2, chips, each, prior_width), BF16),
            pltpu.VMEM((chips, each, prior_width), BF16),
            pltpu.VMEM((chips, each, prior_width), BF16),
            pltpu.VMEM((chips - 1, each, prior_width), BF16),
            pltpu.VMEM((2, chips, each, prior_width), BF16),
            pltpu.VMEM((m, rows_of, keys), BF16),
            pltpu.VMEM((m - 1, rows_of, keys), BF16),
            dma, dma, dma((n,)), dma,
            dma((n, 3, 4)), dma((n, 3)), dma((m - 1,)), dma, dma((2,)), dma((2,)),
            dma((chips - 1,)), dma((chips - 1,)), dma((chips - 1,)), dma((chips - 1,)), dma((m - 1,)), dma((m - 1,)),
        ],
        compiler_params=pltpu.CompilerParams(collective_id=0, has_side_effects=True, vmem_limit_bytes=25 * 1024 * 1024),
    )(vectors.reshape(depth, width), prior, old_block, pair_columns, pivots.reshape(1, keys))

def solution(mesh):
    n, m = mesh.shape["gx"], mesh.shape["gy"]

    def local(old_block, vectors, prior, pair_columns, pivots):
        width = vectors.shape[2]
        whole_tiles = width % 256 == 0 and prior.shape[1] % 256 == 0 and prior.shape[0] // m % 256 == 0
        if n % 4 == 0 and n >= 12 and m >= 2 and pivots.shape[0] % (8 * n) == 0 and whole_tiles:
            return fused(n, m, old_block, vectors, prior, pair_columns, pivots)
        return plain(old_block, vectors, prior, pair_columns, pivots)

    placed = (P("gx", "gy"), P(None, "gy", "gx"), P("gx", "gy"), P(("gx", "gy"), None), P())
    return jax.shard_map(
        local,
        mesh=mesh,
        in_specs=placed,
        out_specs=(P("gx", "gy"), P(("gx", "gy"), None)),
        check_vma=False,
    )
```
